32 devices in a mesh: paths: 4 (over x, core), cpty: 8 (over z, y).
Axes of the slice: x: 2, y: 2, z: 4, core: 2. Of those that a mesh axis runs over, the one named last changes fastest.
Arguments:
- factors: bfloat16 [64, 6144], P(None, 'paths'), may hold values from -6 to 6
- loadings: bfloat16 [64, 16384], P(None, 'cpty'), may hold values from -2 to 2
- notional: bfloat16 [16384], P('cpty'), may hold values from 0.25 to 0.796875
- strike: bfloat16 [16384], P('cpty'), may hold values from 2 to 8
- curvature: bfloat16 [16384], P('cpty'), may hold values from 1 to 3
- trade_cpty: int32 [16384], P('cpty'), may hold values from 0 to 1023, as said below
Outputs:
- exposure: bfloat16 [6144, 1024], P('paths', 'cpty')
- moment: float32 [1024, 1024], P('paths', 'cpty')
The draws below stay inside these ranges and needn't reach their ends.
Inputs may be any that keep to these rules, and one draw needn't show every extreme that they name: `trade_cpty`: of the trades in the book of one index of cpty, at most 512 belong to the counterparties numbered k * 128 to (k + 1) * 128 - 1 for any k; in every draw some such k receives exactly 512 from every book.
All inputs are finite; a program needn't handle non-finite values.
Results may differ from the reference program's by a relative error of at most 0.0064.
Values may be sent and summed in bfloat16 or wider, within the bound.
No kernel may reach another device: no remote copies, remote signals or barrier semaphores. Data moves between devices by JAX's collectives and lax.ppermute only.
A program may use at most 128 MiB of HBM per device.

```python
import math
import jax
import jax.numpy as jnp
from jax import lax

F = 64
CP_DEV = 128
TR_DEV = 2048
SLOT = 512
PATHS = 6144
CPTY = 1024
TRADES = 16384


def draw_trade_cpty(key, part):
    block_count = TRADES // TR_DEV
    owner_count = CPTY // CP_DEV
    base = jax.random.fold_in(key, 11)
    key_heavy, key_blocks = jax.random.split(base, 2)
    heavy_owner = jax.random.randint(key_heavy, (), 0, owner_count)

    def one_block(block_key):
        key_slots, key_shuffle, key_local = jax.random.split(block_key, 3)
        others = jax.random.permutation(key_slots, (owner_count - 1) * SLOT)[:TR_DEV - SLOT] // SLOT
        others = others + (others >= heavy_owner).astype(jnp.int32)
        owners = jnp.concatenate([jnp.full((SLOT,), heavy_owner, jnp.int32), others.astype(jnp.int32)])
        owners = jax.random.permutation(key_shuffle, owners)
        local_ids = jax.random.randint(key_local, (TR_DEV,), 0, CP_DEV)
        return owners * CP_DEV + local_ids
    result = jax.vmap(one_block)(jax.random.split(key_blocks, block_count))
    return result.reshape(-1).astype(jnp.int32)


def levels(rng, dims, cuts, low, top_value):
    factor_of = 1.0
    for dim, parts in cuts:
        heights = jax.random.uniform(jax.random.fold_in(jax.random.fold_in(rng, 6), dim), (parts,), jnp.float32, low / len(cuts), top_value / len(cuts))
        factor_of = factor_of * jnp.repeat(jnp.exp(heights), dims[dim] // parts).reshape((-1,) + (1,) * (len(dims) - 1 - dim))
    return factor_of


def normal_values(stream_key, dims, spread, most, cuts=(), held_as=jnp.bfloat16):
    gain = levels(stream_key, dims, cuts, -0.22, 0.18) if cuts else 1.0
    drawn = jax.random.normal(stream_key, dims, jnp.float32) * spread * gain
    return jnp.minimum(jnp.maximum(drawn, -most), most).astype(held_as)


def setup_inputs(seed: int = 0) -> dict:
    streams_of = jax.random.split(jax.random.key(seed), 7)
    return {
        "factors": normal_values(streams_of[0], (F, PATHS), 1.0, 6.0, ((1, 4),)),
        "loadings": normal_values(streams_of[1], (F, TRADES), (F // 9) ** -0.5, 2.0, ((1, 8),)),
        "notional": jnp.clip(jnp.exp(math.log(0.796875) - 1.1592369 * jax.random.uniform(streams_of[2], (TRADES,), jnp.float32) ** levels(streams_of[2], (TRADES,), ((0, 8),), -0.2, 0.2)), 0.25, 0.796875).astype(jnp.bfloat16),
        "strike": jnp.clip(2.0 + 6.0 * jax.random.uniform(streams_of[3], (TRADES,), jnp.float32) ** levels(streams_of[3], (TRADES,), ((0, 8),), -0.2, 0.2), 2.0, 8.0).astype(jnp.bfloat16),
        "curvature": jnp.clip(1.0 + 2.0 * jax.random.uniform(streams_of[4], (TRADES,), jnp.float32) ** levels(streams_of[4], (TRADES,), ((0, 8),), -0.2, 0.2), 1.0, 3.0).astype(jnp.bfloat16),
        "trade_cpty": draw_trade_cpty(jax.random.fold_in(streams_of[6], 71), 0),
    }


def reference(factors, loadings, notional, strike, curvature, trade_cpty):
    block_count = TRADES // TR_DEV
    load_blocks = jnp.transpose(loadings.reshape(F, block_count, TR_DEV), (1, 0, 2))
    note_blocks = notional.reshape(block_count, TR_DEV)
    strike_blocks = strike.reshape(block_count, TR_DEV)
    curve_blocks = curvature.reshape(block_count, TR_DEV)
    cpty_blocks = trade_cpty.reshape(block_count, TR_DEV).astype(jnp.int32)
    drivers = jnp.transpose(factors)

    def accumulate(carried, pieces):
        loading_cols, note_part, strike_part, curve_part, cpty_ids = pieces
        linear = jnp.dot(drivers, loading_cols, preferred_element_type=jnp.float32)
        value = note_part.astype(jnp.float32) * (linear + curve_part.astype(jnp.float32) * jnp.tanh(linear - strike_part.astype(jnp.float32)))
        value = value.astype(jnp.bfloat16)
        netted_part = jax.ops.segment_sum(jnp.transpose(value.astype(jnp.float32)), cpty_ids, num_segments=CPTY)
        return carried + netted_part, None

    start_sum = jnp.zeros((CPTY, PATHS), jnp.float32)
    netted_rows, _ = lax.scan(accumulate, start_sum, (load_blocks, note_blocks, strike_blocks, curve_blocks, cpty_blocks))
    exposure = jnp.maximum(jnp.transpose(netted_rows), 0.0).astype(jnp.bfloat16)
    moment = jnp.dot(jnp.transpose(exposure), exposure, preferred_element_type=jnp.float32) / PATHS
    return exposure, moment
```

```python
import functools

import jax
import jax.numpy as jnp
from jax import lax
from jax.experimental import pallas as pl
from jax.experimental.pallas import tpu as pltpu
from jax.sharding import PartitionSpec as P

CP_DEV = 128
LANES = 128
SUBLANES = 8

VMEM = pl.BlockSpec(memory_space=pltpu.VMEM)
SMEM = pl.BlockSpec(memory_space=pltpu.SMEM)


def dot_nt(left, right):
    return lax.dot_general(left, right, (((1,), (1,)), ((), ())), preferred_element_type=jnp.float32)


def dot_tn(left, right):
    return lax.dot_general(left, right, (((0,), (0,)), ((), ())), preferred_element_type=jnp.float32)


def pack_kernel(core_ref, ids_ref, loadings_ref, terms_ref, out_ref, described_ref):
    groups, rows, half = out_ref.shape
    factor_count, trades = loadings_ref.shape
    ids = ids_ref[...]
    owners = ids // CP_DEV
    marked = lax.broadcasted_iota(jnp.int32, (groups, trades), 0) == owners
    ones = jnp.where(marked, 1.0, 0.0).astype(jnp.bfloat16)
    blocks = trades // LANES
    stacked = jnp.concatenate([ones[:, b * LANES:(b + 1) * LANES] for b in range(blocks)], axis=0)
    upper = lax.broadcasted_iota(jnp.int32, (LANES, LANES), 0) <= lax.broadcasted_iota(jnp.int32, (LANES, LANES), 1)
    counts = jnp.dot(stacked, jnp.where(upper, 1.0, 0.0).astype(jnp.bfloat16), preferred_element_type=jnp.float32)
    before = jnp.zeros((groups, 1), jnp.float32)
    ranks = []
    for b in range(blocks):
        counted = counts[b * groups:(b + 1) * groups] + before
        chosen = jnp.where(marked[:, b * LANES:(b + 1) * LANES], counted, 0.0)
        ranks.append(jnp.sum(chosen, axis=0, keepdims=True))
        before = counted[:, LANES - 1:]
    ranking = jnp.concatenate(ranks, axis=1).astype(jnp.int32) - 1 - core_ref[0] * half
    target = jnp.where((ranking >= 0) & (ranking < half), owners * half + ranking, -1)
    described_ref[0:factor_count, :] = loadings_ref[...]
    terms = terms_ref[...].astype(jnp.float32)
    local_ids = (ids - owners * CP_DEV).astype(jnp.float32)
    tail = jnp.concatenate([terms, local_ids, jnp.zeros((SUBLANES - 4, trades), jnp.float32)], axis=0)
    described_ref[factor_count:rows, :] = tail.astype(jnp.bfloat16)
    described = described_ref[...]
    for g in range(groups):
        slots = lax.broadcasted_iota(jnp.int32, (half, trades), 0) + g * half
        select = jnp.where(slots == target, 1.0, 0.0).astype(jnp.bfloat16)
        out_ref[g] = dot_nt(described, select).astype(jnp.bfloat16)


def price_kernel(drivers_ref, mine_ref, other_ref, out_ref):
    path_tile = drivers_ref.shape[0]
    factor_count = drivers_ref.shape[1]
    groups, _, half = mine_ref.shape
    drivers = drivers_ref[...]
    total = jnp.zeros((path_tile, CP_DEV), jnp.float32)
    for ref in (mine_ref, other_ref):
        for g in range(groups):
            slab = ref[g]
            terms = slab[factor_count:factor_count + SUBLANES].astype(jnp.float32)
            linear = jnp.dot(drivers, slab[:factor_count], preferred_element_type=jnp.float32)
            value = terms[0:1] * (linear + terms[2:3] * jnp.tanh(linear - terms[1:2]))
            ids = terms[3:4].astype(jnp.int32)
            onehot = jnp.where(lax.broadcasted_iota(jnp.int32, (CP_DEV, half), 0) == ids, 1.0, 0.0)
            total = total + dot_nt(value.astype(jnp.bfloat16), onehot.astype(jnp.bfloat16))
    out_ref[...] = jnp.maximum(total, 0.0).astype(jnp.bfloat16)


def moment_kernel(z_ref, own_ref, peers_ref, whole_ref, half_ref, out_ref, columns_ref):
    lines, block, _ = out_ref.shape
    paths = own_ref.shape[0]
    z = z_ref[0]
    columns_ref[:, 0:block] = own_ref[...]
    for e in range(peers_ref.shape[0]):
        columns_ref[:, (e + 1) * block:(e + 2) * block] = peers_ref[e]
    out_ref[...] = jnp.zeros(out_ref.shape, out_ref.dtype)
    columns = columns_ref[...]
    out_ref[z] = dot_tn(own_ref[...], columns).astype(out_ref.dtype)
    for d in range(1, lines // 2):
        out_ref[(z - d) % lines] = dot_tn(whole_ref[d - 1], columns).astype(out_ref.dtype)
    far = lines // 2
    start = jnp.where(z >= far, 0, paths // 2)
    facing = columns_ref[pl.ds(pl.multiple_of(start, SUBLANES), paths // 2), :]
    out_ref[(z + far) % lines] = dot_tn(half_ref[...], facing).astype(out_ref.dtype)


def final_kernel(y_ref, own_ref, swapped_ref, crossed_ref, out_ref, *, scale):
    depth, block, _ = out_ref.shape
    y = y_ref[0]
    for e in range(depth):
        kept = own_ref[:, 0:block] if e == 0 else swapped_ref[e - 1].astype(jnp.float32)
        k = (-e) % depth
        turned = crossed_ref[:, k * block:(k + 1) * block].astype(jnp.float32).T
        out_ref[(y + e) % depth] = (kept + turned) * scale


def on_device(factors, loadings, notional, strike, curvature, trade_cpty, *, path_tile_count):
    lines = lax.axis_size("paths")
    groups = lax.axis_size("cpty")
    depth = groups // lines
    path_index = lax.axis_index("paths")
    own_index = lax.axis_index("cpty")
    z, y = own_index // depth, own_index % depth
    factor_count, trades = loadings.shape
    paths = factors.shape[1]
    half = trades // groups
    rows = factor_count + SUBLANES
    big = pltpu.CompilerParams(vmem_limit_bytes=56 * 1024 * 1024)

    packed = pl.pallas_call(
        pack_kernel,
        out_shape=jax.ShapeDtypeStruct((groups, rows, half), jnp.bfloat16),
        in_specs=[SMEM, VMEM, VMEM, VMEM],
        out_specs=VMEM,
        scratch_shapes=[pltpu.VMEM((rows, trades), jnp.bfloat16)],
        compiler_params=big,
        name="pack",
    )(
        (path_index % 2).astype(jnp.int32)[None],
        trade_cpty[None, :],
        loadings,
        jnp.stack([notional, strike, curvature]),
    )
    mine = lax.all_to_all(packed, "cpty", split_axis=0, concat_axis=0, tiled=True)
    other = lax.ppermute(mine, "paths", [(i, i ^ 1) for i in range(lines)])

    drivers = jnp.transpose(factors)
    path_tile = paths // path_tile_count
    whole_block = pl.BlockSpec((groups, rows, half), lambda i: (0, 0, 0))
    exposure = pl.pallas_call(
        price_kernel,
        grid=(path_tile_count,),
        out_shape=jax.ShapeDtypeStruct((paths, CP_DEV), jnp.bfloat16),
        in_specs=[pl.BlockSpec((path_tile, factor_count), lambda i: (i, 0)), whole_block, whole_block],
        out_specs=pl.BlockSpec((path_tile, CP_DEV), lambda i: (i, 0)),
        compiler_params=big,
        name="price",
    )(drivers, mine, other)

    everyone = range(groups)
    peers = [
        lax.ppermute(exposure, "cpty", [(c, c - c % depth + (c + e) % depth) for c in everyone])
        for e in range(1, depth)
    ]
    wholes = [
        lax.ppermute(exposure, "cpty", [(c, (c + d * depth) % groups) for c in everyone])
        for d in range(1, lines // 2)
    ]
    far = lines // 2
    sent = lax.dynamic_slice_in_dim(exposure, jnp.where(z < far, 0, paths // 2), paths // 2, 0)
    facing = lax.ppermute(sent, "cpty", [(c, (c + far * depth) % groups) for c in everyone])
    partial = pl.pallas_call(
        moment_kernel,
        out_shape=jax.ShapeDtypeStruct((lines, CP_DEV, depth * CP_DEV), jnp.bfloat16),
        in_specs=[SMEM, VMEM, VMEM, VMEM, VMEM],
        out_specs=VMEM,
        scratch_shapes=[pltpu.VMEM((paths, depth * CP_DEV), jnp.bfloat16)],
        compiler_params=big,
        name="moment",
    )(z.astype(jnp.int32)[None], exposure, jnp.stack(peers), jnp.stack(wholes), facing)
    spread = lax.all_to_all(partial, "paths", split_axis=0, concat_axis=0, tiled=True)
    summed = jnp.sum(spread.astype(jnp.float32), axis=0)
    leaving = summed.astype(jnp.bfloat16)

    def flat(p, zz, yy):
        return p * groups + zz * depth + yy

    crossed = lax.ppermute(
        leaving,
        ("paths", "cpty"),
        [
            (flat(a, b, yy), flat(b, a, yy))
            for a in range(lines)
            for b in range(lines)
            for yy in range(depth)
            if a != b
        ],
    )
    swapped = [
        lax.ppermute(
            leaving[:, e * CP_DEV:(e + 1) * CP_DEV],
            "cpty",
            [(c, c - c % depth + (c - e) % depth) for c in everyone],
        )
        for e in range(1, depth)
    ]
    moment = pl.pallas_call(
        functools.partial(final_kernel, scale=1.0 / (paths * lines)),
        out_shape=jax.ShapeDtypeStruct((depth, CP_DEV, CP_DEV), jnp.float32),
        in_specs=[SMEM, VMEM, VMEM, VMEM],
        out_specs=VMEM,
        compiler_params=big,
        name="final",
    )(y.astype(jnp.int32)[None], summed, jnp.stack(swapped), crossed)
    return exposure, moment.reshape(depth * CP_DEV, CP_DEV)


def solution(mesh):
    in_specs = (P(None, "paths"), P(None, "cpty"), P("cpty"), P("cpty"), P("cpty"), P("cpty"))
    out_specs = (P("paths", "cpty"), P("paths", "cpty"))
    return jax.shard_map(
        functools.partial(on_device, path_tile_count=3),
        mesh=mesh,
        in_specs=in_specs,
        out_specs=out_specs,
        check_vma=False,
    )
```

```python
import functools

import jax
import jax.numpy as jnp
from jax import lax
from jax.experimental import pallas as pl
from jax.experimental.pallas import tpu as pltpu
from jax.sharding import PartitionSpec as P

CP_DEV = 128
LANES = 128
SUBLANES = 8
CORES = 2
CHUNKS = 2

VMEM = pl.BlockSpec(memory_space=pltpu.VMEM)
SMEM = pl.BlockSpec(memory_space=pltpu.SMEM)
HBM = pl.BlockSpec(memory_space=pltpu.HBM)
BIG = pltpu.CompilerParams(vmem_limit_bytes=48 * 1024 * 1024)


def dot_nt(left, right):
    return lax.dot_general(left, right, (((1,), (1,)), ((), ())), preferred_element_type=jnp.float32)


def dot_tn(left, right):
    return lax.dot_general(left, right, (((0,), (0,)), ((), ())), preferred_element_type=jnp.float32)


def near(array):
    return pltpu.with_memory_space_constraint(array, pltpu.VMEM)


def as_row(blocks):
    return jnp.concatenate([blocks[b:b + 1] for b in range(blocks.shape[0])], axis=1)


def pack_kernel(core_ref, ids_hbm, loadings_hbm, notional_hbm, strike_hbm, curvature_hbm, out_ref, described_ref, ids_ref, terms_ref, sems):
    groups, rows, half = out_ref.shape
    factor_count, trades = loadings_hbm.shape
    copies = [pltpu.make_async_copy(ids_hbm, ids_ref, sems.at[0])]
    for i, source in enumerate((notional_hbm, strike_hbm, curvature_hbm)):
        copies.append(pltpu.make_async_copy(source, terms_ref.at[i], sems.at[1 + i]))
    copies.append(pltpu.make_async_copy(loadings_hbm, described_ref.at[0:factor_count], sems.at[4]))
    for copy in copies:
        copy.start()
    copies[0].wait()
    ids = as_row(ids_ref[...])
    owners = ids // CP_DEV
    marked = lax.broadcasted_iota(jnp.int32, (groups, trades), 0) == owners
    ones = jnp.where(marked, 1.0, 0.0).astype(jnp.bfloat16)
    blocks = trades // LANES
    stacked = jnp.concatenate([ones[:, b * LANES:(b + 1) * LANES] for b in range(blocks)], axis=0)
    upper = lax.broadcasted_iota(jnp.int32, (LANES, LANES), 0) <= lax.broadcasted_iota(jnp.int32, (LANES, LANES), 1)
    counts = jnp.dot(stacked, jnp.where(upper, 1.0, 0.0).astype(jnp.bfloat16), preferred_element_type=jnp.float32)
    before = jnp.zeros((groups, 1), jnp.float32)
    ranks = []
    for b in range(blocks):
        counted = counts[b * groups:(b + 1) * groups] + before
        chosen = jnp.where(marked[:, b * LANES:(b + 1) * LANES], counted, 0.0)
        ranks.append(jnp.sum(chosen, axis=0, keepdims=True))
        before = counted[:, LANES - 1:]
    ranking = jnp.concatenate(ranks, axis=1).astype(jnp.int32) - 1 - core_ref[0] * half
    here = (ranking >= 0) & (ranking < half)
    local_ids = (ids - owners * CP_DEV).astype(jnp.float32)
    for copy in copies[1:4]:
        copy.wait()
    terms = [as_row(terms_ref[i].astype(jnp.float32)) for i in range(3)]
    tail = jnp.concatenate(terms + [local_ids, jnp.zeros((SUBLANES - 4, trades), jnp.float32)], axis=0)
    described_ref[factor_count:rows, :] = tail.astype(jnp.bfloat16)
    copies[4].wait()
    described = described_ref[...]
    slots = lax.broadcasted_iota(jnp.int32, (half, LANES), 0).astype(jnp.float32).astype(jnp.bfloat16)
    for g in range(groups):
        target = jnp.where(here & (owners == g), ranking, -1).astype(jnp.float32).astype(jnp.bfloat16)
        select = jnp.concatenate(
            [
                jnp.where(slots == target[:, b * LANES:(b + 1) * LANES], jnp.bfloat16(1), jnp.bfloat16(0))
                for b in range(blocks)
            ],
            axis=1,
        )
        out_ref[g] = dot_nt(described, select).astype(jnp.bfloat16)


def price_kernel(z_ref, drivers_ref, mine_ref, other_ref, own_ref, far_ref, *, chunk, lines):
    paths = own_ref.shape[0]
    factor_count = drivers_ref.shape[1]
    groups, _, half = mine_ref.shape
    drivers = drivers_ref[chunk * paths:(chunk + 1) * paths]
    total = jnp.zeros((paths, CP_DEV), jnp.float32)
    for ref in (mine_ref, other_ref):
        for g in range(groups):
            slab = ref[g]
            terms = slab[factor_count:].astype(jnp.float32)
            linear = jnp.dot(drivers, slab[:factor_count], preferred_element_type=jnp.float32)
            value = terms[0:1] * (linear + terms[2:3] * jnp.tanh(linear - terms[1:2]))
            ids = terms[3:4].astype(jnp.int32)
            onehot = jnp.where(lax.broadcasted_iota(jnp.int32, (CP_DEV, half), 0) == ids, 1.0, 0.0)
            total = total + dot_nt(value.astype(jnp.bfloat16), onehot.astype(jnp.bfloat16))
    own_ref[...] = jnp.maximum(total, 0.0).astype(jnp.bfloat16)
    start = jnp.where(z_ref[0] < lines // 2, 0, paths // 2)
    far_ref[...] = own_ref[pl.ds(pl.multiple_of(start, LANES), paths // 2), :]


def products(z, own_ref, peer_refs, whole_refs, facing_ref, columns_ref, lines):
    paths, block = own_ref.shape
    columns_ref[:, 0:block] = own_ref[...]
    for e, ref in enumerate(peer_refs):
        columns_ref[:, (e + 1) * block:(e + 2) * block] = ref[...]
    columns = columns_ref[...]
    found = [dot_tn(own_ref[...], columns)]
    found += [dot_tn(ref[...], columns) for ref in whole_refs]
    start = jnp.where(z >= lines // 2, 0, paths // 2)
    facing = columns_ref[pl.ds(pl.multiple_of(start, LANES), paths // 2), :]
    return found + [dot_tn(facing_ref[...], facing)]


def first_kernel(place_ref, own_ref, *refs, lines, depth):
    peer_refs, whole_refs = refs[:depth - 1], refs[depth - 1:depth - 1 + lines // 2 - 1]
    facing_ref, out_ref, columns_ref = refs[-3:]
    for d, product in enumerate(products(place_ref[0], own_ref, peer_refs, whole_refs, facing_ref, columns_ref, lines)):
        out_ref[d] = product


def second_kernel(place_ref, before_ref, own_ref, *refs, lines, depth):
    peer_refs, whole_refs = refs[:depth - 1], refs[depth - 1:depth - 1 + lines // 2 - 1]
    facing_ref, kept_ref, sent_ref, columns_ref, all_ref = refs[-5:]
    z, core = place_ref[0], place_ref[1]
    all_ref[...] = jnp.zeros(all_ref.shape, jnp.float32)
    for d, product in enumerate(products(z, own_ref, peer_refs, whole_refs, facing_ref, columns_ref, lines)):
        all_ref[(z - d + lines) % lines] = before_ref[d] + product
    for i in range(lines // CORES):
        kept_ref[i] = all_ref[i * CORES + core]
        sent_ref[i] = all_ref[i * CORES + (1 - core)].astype(jnp.bfloat16)


def cores_kernel(x_ref, kept_ref, came_ref, own_ref, *sent_refs):
    x, count = x_ref[0], kept_ref.shape[0]
    own_ref[...] = kept_ref[x] + came_ref[x].astype(jnp.float32)
    for e, ref in enumerate(sent_refs):
        i = (x + 1 + e) % count
        ref[...] = (kept_ref[i] + came_ref[i].astype(jnp.float32)).astype(jnp.bfloat16)


def chips_kernel(own_ref, *refs, count):
    total = own_ref[...]
    for ref in refs[:count]:
        total = total + ref[...].astype(jnp.float32)
    refs[count][...] = total
    leaving = total.astype(jnp.bfloat16)
    refs[count + 1][...] = leaving
    block = own_ref.shape[0]
    for e, ref in enumerate(refs[count + 2:]):
        ref[...] = leaving[:, (e + 1) * block:(e + 2) * block]


def final_kernel(y_ref, own_ref, crossed_ref, *refs, scale):
    swapped_refs, out_ref = refs[:-1], refs[-1]
    depth, block, _ = out_ref.shape
    y = y_ref[0]
    for e in range(depth):
        kept = own_ref[:, 0:block] if e == 0 else swapped_refs[e - 1][...].astype(jnp.float32)
        k = (-e) % depth
        turned = crossed_ref[:, k * block:(k + 1) * block].astype(jnp.float32).T
        out_ref[(y + e) % depth] = (kept + turned) * scale


def on_device(factors, loadings, notional, strike, curvature, trade_cpty):
    lines = lax.axis_size("paths")
    groups = lax.axis_size("cpty")
    depth = groups // lines
    chips = lines // CORES
    far = lines // 2
    path_index = lax.axis_index("paths").astype(jnp.int32)
    own_index = lax.axis_index("cpty").astype(jnp.int32)
    x, core = path_index // CORES, path_index % CORES
    z, y = own_index // depth, own_index % depth
    factor_count, trades = loadings.shape
    paths = factors.shape[1]
    half = trades // groups
    rows = factor_count + SUBLANES
    blocks = trades // LANES
    width = depth * CP_DEV
    place = jnp.stack([z, core])

    packed = pl.pallas_call(
        pack_kernel,
        out_shape=pltpu.VMEM((groups, rows, half), jnp.bfloat16),
        in_specs=[SMEM] + [HBM] * 5,
        out_specs=VMEM,
        scratch_shapes=[
            pltpu.VMEM((rows, trades), jnp.bfloat16),
            pltpu.VMEM((blocks, LANES), jnp.int32),
            pltpu.VMEM((3, blocks, LANES), jnp.bfloat16),
            pltpu.SemaphoreType.DMA((5,)),
        ],
        compiler_params=BIG,
        name="pack",
    )(
        core[None],
        trade_cpty.reshape(blocks, LANES),
        loadings,
        notional.reshape(blocks, LANES),
        strike.reshape(blocks, LANES),
        curvature.reshape(blocks, LANES),
    )
    mine = lax.all_to_all(packed, "cpty", split_axis=0, concat_axis=0, tiled=True)
    other = lax.ppermute(mine, "paths", [(i, i ^ 1) for i in range(lines)])

    drivers = near(jnp.transpose(factors))
    everyone = range(groups)
    part = paths // CHUNKS
    owns, met = [], []
    for chunk in range(CHUNKS):
        own, leaving = pl.pallas_call(
            functools.partial(price_kernel, chunk=chunk, lines=lines),
            out_shape=(
                pltpu.VMEM((part, CP_DEV), jnp.bfloat16),
                pltpu.VMEM((part // 2, CP_DEV), jnp.bfloat16),
            ),
            in_specs=[SMEM, VMEM, VMEM, VMEM],
            out_specs=(VMEM, VMEM),
            compiler_params=BIG,
            name=f"price{chunk}",
        )(z[None], drivers, near(mine), near(other))
        peers = [
            lax.ppermute(own, "cpty", [(c, c - c % depth + (c + e) % depth) for c in everyone])
            for e in range(1, depth)
        ]
        wholes = [
            lax.ppermute(own, "cpty", [(c, (c + d * depth) % groups) for c in everyone])
            for d in range(1, far)
        ]
        facing = lax.ppermute(leaving, "cpty", [(c, (c + far * depth) % groups) for c in everyone])
        owns.append(own)
        met.append([near(a) for a in [own, *peers, *wholes, facing]])

    count = len(met[0])
    columns = pltpu.VMEM((part, width), jnp.bfloat16)
    before = pl.pallas_call(
        functools.partial(first_kernel, lines=lines, depth=depth),
        out_shape=pltpu.VMEM((far + 1, CP_DEV, width), jnp.float32),
        in_specs=[SMEM] + [VMEM] * count,
        out_specs=VMEM,
        scratch_shapes=[columns],
        compiler_params=BIG,
        name="moment0",
    )(place, *met[0])
    kept, sent = pl.pallas_call(
        functools.partial(second_kernel, lines=lines, depth=depth),
        out_shape=(
            pltpu.VMEM((chips, CP_DEV, width), jnp.float32),
            pltpu.VMEM((chips, CP_DEV, width), jnp.bfloat16),
        ),
        in_specs=[SMEM] + [VMEM] * (count + 1),
        out_specs=(VMEM, VMEM),
        scratch_shapes=[columns, pltpu.VMEM((lines, CP_DEV, width), jnp.float32)],
        compiler_params=BIG,
        name="moment1",
    )(place, near(before), *met[1])
    came = lax.ppermute(sent, "paths", [(i, i ^ 1) for i in range(lines)])
    out = pl.pallas_call(
        cores_kernel,
        out_shape=[pltpu.VMEM((CP_DEV, width), jnp.float32)]
        + [pltpu.VMEM((CP_DEV, width), jnp.bfloat16)] * (chips - 1),
        in_specs=[SMEM, VMEM, VMEM],
        out_specs=[VMEM] * chips,
        compiler_params=BIG,
        name="cores",
    )(x[None], near(kept), near(came))
    arrived = [
        lax.ppermute(out[e], "paths", [(i, (i + e * CORES) % lines) for i in range(lines)])
        for e in range(1, chips)
    ]
    total, leaving, *swaps = pl.pallas_call(
        functools.partial(chips_kernel, count=chips - 1),
        out_shape=[
            pltpu.VMEM((CP_DEV, width), jnp.float32),
            pltpu.VMEM((CP_DEV, width), jnp.bfloat16),
        ]
        + [pltpu.VMEM((CP_DEV, CP_DEV), jnp.bfloat16)] * (depth - 1),
        in_specs=[VMEM] * chips,
        out_specs=[VMEM] * (depth + 1),
        compiler_params=BIG,
        name="chips",
    )(near(out[0]), *[near(a) for a in arrived])

    def flat(p, zz, yy):
        return p * groups + zz * depth + yy

    crossed = lax.ppermute(
        leaving,
        ("paths", "cpty"),
        [
            (flat(a, b, yy), flat(b, a, yy))
            for a in range(lines)
            for b in range(lines)
            for yy in range(depth)
            if a != b
        ],
    )
    swapped = [
        lax.ppermute(swaps[e - 1], "cpty", [(c, c - c % depth + (c - e) % depth) for c in everyone])
        for e in range(1, depth)
    ]
    moment = pl.pallas_call(
        functools.partial(final_kernel, scale=1.0 / (paths * lines)),
        out_shape=jax.ShapeDtypeStruct((depth, CP_DEV, CP_DEV), jnp.float32),
        in_specs=[SMEM] + [VMEM] * (depth + 1),
        out_specs=VMEM,
        compiler_params=BIG,
        name="final",
    )(y[None], near(total), near(crossed), *[near(a) for a in swapped])
    return jnp.concatenate(owns, axis=0), moment.reshape(depth * CP_DEV, CP_DEV)


def solution(mesh):
    in_specs = (P(None, "paths"), P(None, "cpty"), P("cpty"), P("cpty"), P("cpty"), P("cpty"))
    out_specs = (P("paths", "cpty"), P("paths", "cpty"))
    return jax.shard_map(on_device, mesh=mesh, in_specs=in_specs, out_specs=out_specs, check_vma=False)
```

```python
import functools

import jax
import jax.numpy as jnp
from jax import lax
from jax.experimental import pallas as pl
from jax.experimental.pallas import tpu as pltpu
from jax.sharding import PartitionSpec as P

CP_DEV = 128
LANES = 128
SUBLANES = 8
CORES = 2
CHUNKS = 2

VMEM = pl.BlockSpec(memory_space=pltpu.VMEM)
SMEM = pl.BlockSpec(memory_space=pltpu.SMEM)
HBM = pl.BlockSpec(memory_space=pltpu.HBM)
BIG = pltpu.CompilerParams(vmem_limit_bytes=48 * 1024 * 1024)


def dot_nt(left, right):
    return lax.dot_general(left, right, (((1,), (1,)), ((), ())), preferred_element_type=jnp.float32)


def dot_tn(left, right):
    return lax.dot_general(left, right, (((0,), (0,)), ((), ())), preferred_element_type=jnp.float32)


def near(array):
    return pltpu.with_memory_space_constraint(array, pltpu.VMEM)


def outside(array):
    return pltpu.with_memory_space_constraint(array, pltpu.HBM)


def as_row(blocks):
    return jnp.concatenate([blocks[b:b + 1] for b in range(blocks.shape[0])], axis=1)


def pack_kernel(core_ref, ids_hbm, loadings_hbm, notional_hbm, strike_hbm, curvature_hbm, out_ref, described_ref, ids_ref, terms_ref, sems):
    groups, rows, half = out_ref.shape
    factor_count, trades = loadings_hbm.shape
    copies = [pltpu.make_async_copy(ids_hbm, ids_ref, sems.at[0])]
    for i, source in enumerate((notional_hbm, strike_hbm, curvature_hbm)):
        copies.append(pltpu.make_async_copy(source, terms_ref.at[i], sems.at[1 + i]))
    copies.append(pltpu.make_async_copy(loadings_hbm, described_ref.at[0:factor_count], sems.at[4]))
    for copy in copies:
        copy.start()
    copies[0].wait()
    ids = as_row(ids_ref[...])
    owners = ids // CP_DEV
    marked = lax.broadcasted_iota(jnp.int32, (groups, trades), 0) == owners
    ones = jnp.where(marked, 1.0, 0.0).astype(jnp.bfloat16)
    blocks = trades // LANES
    stacked = jnp.concatenate([ones[:, b * LANES:(b + 1) * LANES] for b in range(blocks)], axis=0)
    row = lax.broadcasted_iota(jnp.int32, (LANES, 2 * LANES), 0)
    lane = lax.broadcasted_iota(jnp.int32, (LANES, 2 * LANES), 1)
    upto = jnp.where((row <= lane) | (lane >= LANES), 1.0, 0.0).astype(jnp.bfloat16)
    counts = jnp.dot(stacked, upto, preferred_element_type=jnp.float32)
    size = blocks * groups
    late = lax.broadcasted_iota(jnp.int32, (size, size), 0)
    early = lax.broadcasted_iota(jnp.int32, (size, size), 1)
    earlier = jnp.where((late % groups == early % groups) & (early < late), 1.0, 0.0).astype(jnp.bfloat16)
    before = jnp.dot(earlier, counts[:, LANES:].astype(jnp.bfloat16), preferred_element_type=jnp.float32)
    counted = counts[:, :LANES] + before
    ranks = []
    for b in range(blocks):
        chosen = jnp.where(marked[:, b * LANES:(b + 1) * LANES], counted[b * groups:(b + 1) * groups], 0.0)
        ranks.append(jnp.sum(chosen, axis=0, keepdims=True))
    ranking = jnp.concatenate(ranks, axis=1).astype(jnp.int32) - 1 - core_ref[0] * half
    here = (ranking >= 0) & (ranking < half)
    local_ids = (ids - owners * CP_DEV).astype(jnp.float32)
    for copy in copies[1:4]:
        copy.wait()
    terms = [as_row(terms_ref[i].astype(jnp.float32)) for i in range(3)]
    tail = jnp.concatenate(terms + [local_ids, jnp.zeros((SUBLANES - 4, trades), jnp.float32)], axis=0)
    described_ref[factor_count:rows, :] = tail.astype(jnp.bfloat16)
    copies[4].wait()
    described = described_ref[...]
    slots = lax.broadcasted_iota(jnp.int32, (half, LANES), 0).astype(jnp.float32).astype(jnp.bfloat16)
    for g in range(groups):
        target = jnp.where(here & (owners == g), ranking, -1).astype(jnp.float32).astype(jnp.bfloat16)
        select = jnp.concatenate(
            [
                jnp.where(slots == target[:, b * LANES:(b + 1) * LANES], jnp.bfloat16(1), jnp.bfloat16(0))
                for b in range(blocks)
            ],
            axis=1,
        )
        out_ref[g] = dot_nt(described, select).astype(jnp.bfloat16)


def price_kernel(z_ref, drivers_ref, mine_ref, other_ref, own_ref, far_ref, *, chunk, lines):
    paths = own_ref.shape[0]
    factor_count = drivers_ref.shape[1]
    groups, _, half = mine_ref.shape
    drivers = drivers_ref[chunk * paths:(chunk + 1) * paths]
    total = jnp.zeros((paths, CP_DEV), jnp.float32)
    for ref in (mine_ref, other_ref):
        for g in range(groups):
            slab = ref[g]
            terms = slab[factor_count:].astype(jnp.float32)
            linear = jnp.dot(drivers, slab[:factor_count], preferred_element_type=jnp.float32)
            value = terms[0:1] * (linear + terms[2:3] * jnp.tanh(linear - terms[1:2]))
            ids = terms[3:4].astype(jnp.int32)
            onehot = jnp.where(lax.broadcasted_iota(jnp.int32, (CP_DEV, half), 0) == ids, 1.0, 0.0)
            total = total + dot_nt(value.astype(jnp.bfloat16), onehot.astype(jnp.bfloat16))
    own_ref[...] = jnp.maximum(total, 0.0).astype(jnp.bfloat16)
    start = jnp.where(z_ref[0] < lines // 2, 0, paths // 2)
    far_ref[...] = own_ref[pl.ds(pl.multiple_of(start, LANES), paths // 2), :]


def products(z, own_ref, peer_refs, whole_refs, facing_ref, columns_ref, lines):
    paths, block = own_ref.shape
    columns_ref[:, 0:block] = own_ref[...]
    for e, ref in enumerate(peer_refs):
        columns_ref[:, (e + 1) * block:(e + 2) * block] = ref[...]
    columns = columns_ref[...]
    found = [dot_tn(own_ref[...], columns)]
    found += [dot_tn(ref[...], columns) for ref in whole_refs]
    start = jnp.where(z >= lines // 2, 0, paths // 2)
    facing = columns_ref[pl.ds(pl.multiple_of(start, LANES), paths // 2), :]
    return found + [dot_tn(facing_ref[...], facing)]


def first_kernel(place_ref, own_ref, *refs, lines, depth):
    peer_refs, whole_refs = refs[:depth - 1], refs[depth - 1:depth - 1 + lines // 2 - 1]
    facing_ref, out_ref, columns_ref = refs[-3:]
    for d, product in enumerate(products(place_ref[0], own_ref, peer_refs, whole_refs, facing_ref, columns_ref, lines)):
        out_ref[d] = product


def second_kernel(place_ref, before_ref, own_ref, *refs, lines, depth):
    peer_refs, whole_refs = refs[:depth - 1], refs[depth - 1:depth - 1 + lines // 2 - 1]
    facing_ref, kept_ref, sent_ref, columns_ref, all_ref = refs[-5:]
    z, core = place_ref[0], place_ref[1]
    all_ref[...] = jnp.zeros(all_ref.shape, jnp.float32)
    for d, product in enumerate(products(z, own_ref, peer_refs, whole_refs, facing_ref, columns_ref, lines)):
        all_ref[(z - d + lines) % lines] = before_ref[d] + product
    for i in range(lines // CORES):
        kept_ref[i] = all_ref[i * CORES + core]
        sent_ref[i] = all_ref[i * CORES + (1 - core)].astype(jnp.bfloat16)


def cores_kernel(x_ref, kept_ref, came_ref, own_ref, *sent_refs):
    x, count = x_ref[0], kept_ref.shape[0]
    own_ref[...] = kept_ref[x] + came_ref[x].astype(jnp.float32)
    for e, ref in enumerate(sent_refs):
        i = (x + 1 + e) % count
        ref[...] = (kept_ref[i] + came_ref[i].astype(jnp.float32)).astype(jnp.bfloat16)


def chips_kernel(own_ref, *refs, count):
    total = own_ref[...]
    for ref in refs[:count]:
        total = total + ref[...].astype(jnp.float32)
    refs[count][...] = total
    leaving = total.astype(jnp.bfloat16)
    refs[count + 1][...] = leaving
    block = own_ref.shape[0]
    for e, ref in enumerate(refs[count + 2:]):
        ref[...] = leaving[:, (e + 1) * block:(e + 2) * block]


def final_kernel(y_ref, own_ref, crossed_ref, *refs, scale):
    swapped_refs, out_ref = refs[:-1], refs[-1]
    depth, block, _ = out_ref.shape
    y = y_ref[0]
    for e in range(depth):
        kept = own_ref[:, 0:block] if e == 0 else swapped_refs[e - 1][...].astype(jnp.float32)
        k = (-e) % depth
        turned = crossed_ref[:, k * block:(k + 1) * block].astype(jnp.float32).T
        out_ref[(y + e) % depth] = (kept + turned) * scale


def on_device(factors, loadings, notional, strike, curvature, trade_cpty):
    lines = lax.axis_size("paths")
    groups = lax.axis_size("cpty")
    depth = groups // lines
    chips = lines // CORES
    far = lines // 2
    path_index = lax.axis_index("paths").astype(jnp.int32)
    own_index = lax.axis_index("cpty").astype(jnp.int32)
    x, core = path_index // CORES, path_index % CORES
    z, y = own_index // depth, own_index % depth
    factor_count, trades = loadings.shape
    paths = factors.shape[1]
    half = trades // groups
    rows = factor_count + SUBLANES
    blocks = trades // LANES
    width = depth * CP_DEV
    place = jnp.stack([z, core])

    packed = pl.pallas_call(
        pack_kernel,
        out_shape=pltpu.VMEM((groups, rows, half), jnp.bfloat16),
        in_specs=[SMEM] + [HBM] * 5,
        out_specs=VMEM,
        scratch_shapes=[
            pltpu.VMEM((rows, trades), jnp.bfloat16),
            pltpu.VMEM((blocks, LANES), jnp.int32),
            pltpu.VMEM((3, blocks, LANES), jnp.bfloat16),
            pltpu.SemaphoreType.DMA((5,)),
        ],
        compiler_params=BIG,
        name="pack",
    )(
        core[None],
        outside(trade_cpty.reshape(blocks, LANES)),
        outside(loadings),
        outside(notional.reshape(blocks, LANES)),
        outside(strike.reshape(blocks, LANES)),
        outside(curvature.reshape(blocks, LANES)),
    )
    mine = lax.all_to_all(packed, "cpty", split_axis=0, concat_axis=0, tiled=True)
    other = lax.ppermute(mine, "paths", [(i, i ^ 1) for i in range(lines)])

    drivers = near(jnp.transpose(factors))
    everyone = range(groups)
    part = paths // CHUNKS
    owns, met = [], []
    for chunk in range(CHUNKS):
        own, leaving = pl.pallas_call(
            functools.partial(price_kernel, chunk=chunk, lines=lines),
            out_shape=(
                pltpu.VMEM((part, CP_DEV), jnp.bfloat16),
                pltpu.VMEM((part // 2, CP_DEV), jnp.bfloat16),
            ),
            in_specs=[SMEM, VMEM, VMEM, VMEM],
            out_specs=(VMEM, VMEM),
            compiler_params=BIG,
            name=f"price{chunk}",
        )(z[None], drivers, near(mine), near(other))
        peers = [
            lax.ppermute(own, "cpty", [(c, c - c % depth + (c + e) % depth) for c in everyone])
            for e in range(1, depth)
        ]
        wholes = [
            lax.ppermute(own, "cpty", [(c, (c + d * depth) % groups) for c in everyone])
            for d in range(1, far)
        ]
        facing = lax.ppermute(leaving, "cpty", [(c, (c + far * depth) % groups) for c in everyone])
        owns.append(own)
        met.append([near(a) for a in [own, *peers, *wholes, facing]])

    count = len(met[0])
    columns = pltpu.VMEM((part, width), jnp.bfloat16)
    before = pl.pallas_call(
        functools.partial(first_kernel, lines=lines, depth=depth),
        out_shape=pltpu.VMEM((far + 1, CP_DEV, width), jnp.float32),
        in_specs=[SMEM] + [VMEM] * count,
        out_specs=VMEM,
        scratch_shapes=[columns],
        compiler_params=BIG,
        name="moment0",
    )(place, *met[0])
    kept, sent = pl.pallas_call(
        functools.partial(second_kernel, lines=lines, depth=depth),
        out_shape=(
            pltpu.VMEM((chips, CP_DEV, width), jnp.float32),
            pltpu.VMEM((chips, CP_DEV, width), jnp.bfloat16),
        ),
        in_specs=[SMEM] + [VMEM] * (count + 1),
        out_specs=(VMEM, VMEM),
        scratch_shapes=[columns, pltpu.VMEM((lines, CP_DEV, width), jnp.float32)],
        compiler_params=BIG,
        name="moment1",
    )(place, near(before), *met[1])
    came = lax.ppermute(sent, "paths", [(i, i ^ 1) for i in range(lines)])
    out = pl.pallas_call(
        cores_kernel,
        out_shape=[pltpu.VMEM((CP_DEV, width), jnp.float32)]
        + [pltpu.VMEM((CP_DEV, width), jnp.bfloat16)] * (chips - 1),
        in_specs=[SMEM, VMEM, VMEM],
        out_specs=[VMEM] * chips,
        compiler_params=BIG,
        name="cores",
    )(x[None], near(kept), near(came))
    arrived = [
        lax.ppermute(out[e], "paths", [(i, (i + e * CORES) % lines) for i in range(lines)])
        for e in range(1, chips)
    ]
    total, leaving, *swaps = pl.pallas_call(
        functools.partial(chips_kernel, count=chips - 1),
        out_shape=[
            pltpu.VMEM((CP_DEV, width), jnp.float32),
            pltpu.VMEM((CP_DEV, width), jnp.bfloat16),
        ]
        + [pltpu.VMEM((CP_DEV, CP_DEV), jnp.bfloat16)] * (depth - 1),
        in_specs=[VMEM] * chips,
        out_specs=[VMEM] * (depth + 1),
        compiler_params=BIG,
        name="chips",
    )(near(out[0]), *[near(a) for a in arrived])

    def flat(p, zz, yy):
        return p * groups + zz * depth + yy

    crossed = lax.ppermute(
        leaving,
        ("paths", "cpty"),
        [
            (flat(a, b, yy), flat(b, a, yy))
            for a in range(lines)
            for b in range(lines)
            for yy in range(depth)
            if a != b
        ],
    )
    swapped = [
        lax.ppermute(swaps[e - 1], "cpty", [(c, c - c % depth + (c - e) % depth) for c in everyone])
        for e in range(1, depth)
    ]
    moment = pl.pallas_call(
        functools.partial(final_kernel, scale=1.0 / (paths * lines)),
        out_shape=jax.ShapeDtypeStruct((depth, CP_DEV, CP_DEV), jnp.float32),
        in_specs=[SMEM] + [VMEM] * (depth + 1),
        out_specs=VMEM,
        compiler_params=BIG,
        name="final",
    )(y[None], near(total), near(crossed), *[near(a) for a in swapped])
    return jnp.concatenate(owns, axis=0), moment.reshape(depth * CP_DEV, CP_DEV)


def solution(mesh):
    in_specs = (P(None, "paths"), P(None, "cpty"), P("cpty"), P("cpty"), P("cpty"), P("cpty"))
    out_specs = (P("paths", "cpty"), P("paths", "cpty"))
    return jax.shard_map(on_device, mesh=mesh, in_specs=in_specs, out_specs=out_specs, check_vma=False)
```

```python
import functools

import jax
import jax.numpy as jnp
from jax import lax
from jax.experimental import pallas as pl
from jax.experimental.pallas import tpu as pltpu
from jax.sharding import PartitionSpec as P

CP_DEV = 128
LANES = 128
SUBLANES = 8
CORES = 2

VMEM = pl.BlockSpec(memory_space=pltpu.VMEM)
SMEM = pl.BlockSpec(memory_space=pltpu.SMEM)
HBM = pl.BlockSpec(memory_space=pltpu.HBM)
BIG = pltpu.CompilerParams(vmem_limit_bytes=48 * 1024 * 1024)


def dot_nt(left, right):
    return lax.dot_general(left, right, (((1,), (1,)), ((), ())), preferred_element_type=jnp.float32)


def dot_tn(left, right):
    return lax.dot_general(left, right, (((0,), (0,)), ((), ())), preferred_element_type=jnp.float32)


def near(array):
    return pltpu.with_memory_space_constraint(array, pltpu.VMEM)


def outside(array):
    return pltpu.with_memory_space_constraint(array, pltpu.HBM)


def as_row(blocks):
    return jnp.concatenate([blocks[b:b + 1] for b in range(blocks.shape[0])], axis=1)


def pack_kernel(core_ref, ids_hbm, loadings_hbm, notional_hbm, strike_hbm, curvature_hbm, out_ref, described_ref, ids_ref, terms_ref, sems):
    groups, rows, half = out_ref.shape
    factor_count, trades = loadings_hbm.shape
    copies = [pltpu.make_async_copy(ids_hbm, ids_ref, sems.at[0])]
    for i, source in enumerate((notional_hbm, strike_hbm, curvature_hbm)):
        copies.append(pltpu.make_async_copy(source, terms_ref.at[i], sems.at[1 + i]))
    copies.append(pltpu.make_async_copy(loadings_hbm, described_ref.at[0:factor_count], sems.at[4]))
    for copy in copies:
        copy.start()
    copies[0].wait()
    ids = as_row(ids_ref[...])
    owners = ids // CP_DEV
    marked = lax.broadcasted_iota(jnp.int32, (groups, trades), 0) == owners
    ones = jnp.where(marked, 1.0, 0.0).astype(jnp.bfloat16)
    blocks = trades // LANES
    stacked = jnp.concatenate([ones[:, b * LANES:(b + 1) * LANES] for b in range(blocks)], axis=0)
    row = lax.broadcasted_iota(jnp.int32, (LANES, 2 * LANES), 0)
    lane = lax.broadcasted_iota(jnp.int32, (LANES, 2 * LANES), 1)
    upto = jnp.where((row <= lane) | (lane >= LANES), 1.0, 0.0).astype(jnp.bfloat16)
    counts = jnp.dot(stacked, upto, preferred_element_type=jnp.float32)
    size = blocks * groups
    late = lax.broadcasted_iota(jnp.int32, (size, size), 0)
    early = lax.broadcasted_iota(jnp.int32, (size, size), 1)
    earlier = jnp.where((late % groups == early % groups) & (early < late), 1.0, 0.0).astype(jnp.bfloat16)
    before = jnp.dot(earlier, counts[:, LANES:].astype(jnp.bfloat16), preferred_element_type=jnp.float32)
    counted = counts[:, :LANES] + before
    ranks = []
    for b in range(blocks):
        chosen = jnp.where(marked[:, b * LANES:(b + 1) * LANES], counted[b * groups:(b + 1) * groups], 0.0)
        ranks.append(jnp.sum(chosen, axis=0, keepdims=True))
    ranking = jnp.concatenate(ranks, axis=0).astype(jnp.int32) - 1 - core_ref[0] * half
    places = ids_ref[...] // CP_DEV * half + ranking
    places = jnp.where((ranking >= 0) & (ranking < half), places, -2 * trades).astype(jnp.float32).T
    columns = jnp.concatenate(
        [jnp.broadcast_to(places[:, b:b + 1], (LANES, LANES)) for b in range(blocks)], axis=0
    )
    local_ids = (ids - owners * CP_DEV).astype(jnp.float32)
    for copy in copies[1:4]:
        copy.wait()
    terms = [as_row(terms_ref[i].astype(jnp.float32)) for i in range(3)]
    tail = jnp.concatenate(terms + [local_ids, jnp.zeros((SUBLANES - 4, trades), jnp.float32)], axis=0)
    described_ref[factor_count:rows, :] = tail.astype(jnp.bfloat16)
    copies[4].wait()
    described = described_ref[...]
    exact = jnp.bfloat16 if half <= 256 else jnp.float32
    width = min(half, LANES)
    slots = lax.broadcasted_iota(jnp.int32, (trades, half), 1).astype(jnp.float32).astype(exact)
    for g in range(groups):
        target = (columns[:, :width] - float(g * half)).astype(exact)
        select = jnp.concatenate(
            [
                jnp.where(target == slots[:, start:start + width], exact(1), exact(0))
                for start in range(0, half, width)
            ],
            axis=1,
        )
        packed = jnp.dot(described, select.astype(jnp.bfloat16), preferred_element_type=jnp.float32)
        out_ref[g] = packed.astype(jnp.bfloat16)


def net(drivers, ref, total):
    groups, _, half = ref.shape
    factor_count = drivers.shape[1]
    for g in range(groups):
        slab = ref[g]
        terms = slab[factor_count:].astype(jnp.float32)
        linear = jnp.dot(drivers, slab[:factor_count], preferred_element_type=jnp.float32)
        value = terms[0:1] * (linear + terms[2:3] * jnp.tanh(linear - terms[1:2]))
        ids = terms[3:4].astype(jnp.int32)
        onehot = jnp.where(lax.broadcasted_iota(jnp.int32, (CP_DEV, half), 0) == ids, 1.0, 0.0)
        total = total + dot_nt(value.astype(jnp.bfloat16), onehot.astype(jnp.bfloat16))
    return total


def begin_kernel(drivers_ref, mine_ref, out_ref):
    paths = out_ref.shape[0]
    out_ref[...] = net(drivers_ref[0:paths], mine_ref, jnp.zeros((paths, CP_DEV), jnp.float32))


def exposed(total):
    return jnp.maximum(total, 0.0).astype(jnp.bfloat16)


def leaving_half(z_ref, exposure_ref, far_ref, lines):
    paths = far_ref.shape[0]
    start = jnp.where(z_ref[0] < lines // 2, 0, paths)
    far_ref[...] = exposure_ref[pl.ds(pl.multiple_of(start, SUBLANES), paths), :]


def early_kernel(z_ref, drivers_ref, begun_ref, other_ref, out_ref, far_ref, *, lines):
    paths = out_ref.shape[0]
    out_ref[...] = exposed(net(drivers_ref[0:paths], other_ref, begun_ref[...]))
    leaving_half(z_ref, out_ref, far_ref, lines)


def late_kernel(z_ref, drivers_ref, mine_ref, other_ref, out_ref, far_ref, *, lines):
    paths = out_ref.shape[0]
    drivers = drivers_ref[drivers_ref.shape[0] - paths:]
    total = net(drivers, mine_ref, jnp.zeros((paths, CP_DEV), jnp.float32))
    out_ref[...] = exposed(net(drivers, other_ref, total))
    leaving_half(z_ref, out_ref, far_ref, lines)


def products(z, own_ref, facing_ref, peer_refs, whole_refs, columns_ref, lines):
    block = own_ref.shape[1]
    columns_ref[:, 0:block] = own_ref[...]
    for e, ref in enumerate(peer_refs):
        columns_ref[:, (e + 1) * block:(e + 2) * block] = ref[...]
    columns = columns_ref[...]
    found = [dot_tn(ref[...], columns) for ref in (own_ref, *whole_refs)]
    paths = facing_ref.shape[0]
    start = jnp.where(z >= lines // 2, 0, paths)
    facing = columns_ref[pl.ds(pl.multiple_of(start, SUBLANES), paths), :]
    return found + [dot_tn(facing_ref[...], facing)]


def first_kernel(place_ref, late_ref, own_ref, facing_ref, *refs, lines, depth):
    out_ref, exposure_ref, columns_ref = refs[-3:]
    paths = own_ref.shape[0]
    exposure_ref[0:paths] = own_ref[...]
    exposure_ref[paths:] = late_ref[...]
    found = products(place_ref[0], own_ref, facing_ref, refs[:depth - 1], refs[depth - 1:-3], columns_ref, lines)
    for d, product in enumerate(found):
        out_ref[d] = product


def last_kernel(place_ref, before_ref, own_ref, facing_ref, *refs, lines, depth):
    kept_ref, sent_ref, columns_ref, all_ref = refs[-4:]
    z, core = place_ref[0], place_ref[1]
    found = products(z, own_ref, facing_ref, refs[:depth - 1], refs[depth - 1:-4], columns_ref, lines)
    all_ref[...] = jnp.zeros(all_ref.shape, jnp.float32)
    for d, product in enumerate(found):
        all_ref[(z - d + lines) % lines] = before_ref[d] + product
    for i in range(lines // CORES):
        kept_ref[i] = all_ref[i * CORES + core]
        sent_ref[i] = all_ref[i * CORES + (1 - core)].astype(jnp.bfloat16)


def cores_kernel(x_ref, kept_ref, came_ref, own_ref, *sent_refs):
    x, count = x_ref[0], kept_ref.shape[0]
    for e, ref in enumerate(sent_refs):
        i = (x + e) % count
        total = kept_ref[i] + came_ref[i].astype(jnp.float32)
        ref[...] = total.astype(jnp.bfloat16)
        if e == 0:
            own_ref[...] = total


def chips_kernel(own_ref, *refs, count):
    total = own_ref[...]
    for ref in refs[:count]:
        total = total + ref[...].astype(jnp.float32)
    block = own_ref.shape[0]
    refs[count][...] = total[:, 0:block]
    for e, ref in enumerate(refs[count + 1:]):
        ref[...] = total[:, (e + 1) * block:(e + 2) * block].astype(jnp.bfloat16)


def final_kernel(y_ref, own_ref, *refs, scale):
    out_ref = refs[-1]
    depth, block, _ = out_ref.shape
    swapped_refs, crossed_refs = refs[:depth - 1], refs[depth - 1:-1]
    y = y_ref[0]
    for e in range(depth):
        kept = own_ref[...] if e == 0 else swapped_refs[e - 1][...].astype(jnp.float32)
        k = (-e) % depth
        turned = sum(ref[:, k * block:(k + 1) * block].astype(jnp.float32) for ref in crossed_refs).T
        out_ref[(y + e) % depth] = (kept + turned) * scale


def on_device(factors, loadings, notional, strike, curvature, trade_cpty):
    lines = lax.axis_size("paths")
    groups = lax.axis_size("cpty")
    depth = groups // lines
    chips = lines // CORES
    far = lines // 2
    path_index = lax.axis_index("paths").astype(jnp.int32)
    own_index = lax.axis_index("cpty").astype(jnp.int32)
    x, core = path_index // CORES, path_index % CORES
    z, y = own_index // depth, own_index % depth
    factor_count, trades = loadings.shape
    paths = factors.shape[1]
    half = trades // groups
    rows = factor_count + SUBLANES
    blocks = trades // LANES
    width = depth * CP_DEV
    place = jnp.stack([z, core])

    packed = pl.pallas_call(
        pack_kernel,
        out_shape=pltpu.VMEM((groups, rows, half), jnp.bfloat16),
        in_specs=[SMEM] + [HBM] * 5,
        out_specs=VMEM,
        scratch_shapes=[
            pltpu.VMEM((rows, trades), jnp.bfloat16),
            pltpu.VMEM((blocks, LANES), jnp.int32),
            pltpu.VMEM((3, blocks, LANES), jnp.bfloat16),
            pltpu.SemaphoreType.DMA((5,)),
        ],
        compiler_params=BIG,
        name="pack",
    )(
        core[None],
        outside(trade_cpty.reshape(blocks, LANES)),
        outside(loadings),
        outside(notional.reshape(blocks, LANES)),
        outside(strike.reshape(blocks, LANES)),
        outside(curvature.reshape(blocks, LANES)),
    )
    mine = lax.all_to_all(packed, "cpty", split_axis=0, concat_axis=0, tiled=True)
    other = lax.ppermute(mine, "paths", [(i, i ^ 1) for i in range(lines)])

    drivers = near(jnp.transpose(factors))
    everyone = range(groups)
    parts = [paths * 5 // 12 // 32 * 32]
    parts.append(paths - parts[0])
    mine, other = near(mine), near(other)
    begun = pl.pallas_call(
        begin_kernel,
        out_shape=pltpu.VMEM((parts[0], CP_DEV), jnp.float32),
        in_specs=[VMEM, VMEM],
        out_specs=VMEM,
        compiler_params=BIG,
        name="begin",
    )(drivers, mine)

    def priced(kernel, i, *operands):
        return pl.pallas_call(
            functools.partial(kernel, lines=lines),
            out_shape=(
                pltpu.VMEM((parts[i], CP_DEV), jnp.bfloat16),
                pltpu.VMEM((parts[i] // 2, CP_DEV), jnp.bfloat16),
            ),
            in_specs=[SMEM] + [VMEM] * (1 + len(operands)),
            out_specs=[VMEM] * 2,
            compiler_params=BIG,
        )(z[None], drivers, *operands)

    def sent_round(own, leaving):
        def send(array, pairs):
            return near(lax.ppermute(array, "cpty", pairs))

        facing = send(leaving, [(c, (c + far * depth) % groups) for c in everyone])
        wholes = [send(own, [(c, (c + d * depth) % groups) for c in everyone]) for d in range(1, far)]
        peers = [send(own, [(c, c - c % depth + (c + e) % depth) for c in everyone]) for e in range(1, depth)]
        return [near(own), facing, *peers, *wholes]

    early, leaving = priced(early_kernel, 0, near(begun), other)
    early_met = sent_round(early, leaving)
    late, leaving = priced(late_kernel, 1, mine, other)
    late_met = sent_round(late, leaving)
    before, exposure = pl.pallas_call(
        functools.partial(first_kernel, lines=lines, depth=depth),
        out_shape=(
            pltpu.VMEM((far + 1, CP_DEV, width), jnp.float32),
            jax.ShapeDtypeStruct((paths, CP_DEV), jnp.bfloat16),
        ),
        in_specs=[SMEM] + [VMEM] * (1 + len(early_met)),
        out_specs=[VMEM] * 2,
        scratch_shapes=[pltpu.VMEM((parts[0], width), jnp.bfloat16)],
        compiler_params=BIG,
        name="first",
    )(place, near(late), *early_met)
    kept, sent = pl.pallas_call(
        functools.partial(last_kernel, lines=lines, depth=depth),
        out_shape=(
            pltpu.VMEM((chips, CP_DEV, width), jnp.float32),
            pltpu.VMEM((chips, CP_DEV, width), jnp.bfloat16),
        ),
        in_specs=[SMEM] + [VMEM] * (1 + len(late_met)),
        out_specs=(VMEM, VMEM),
        scratch_shapes=[
            pltpu.VMEM((parts[1], width), jnp.bfloat16),
            pltpu.VMEM((lines, CP_DEV, width), jnp.float32),
        ],
        compiler_params=BIG,
        name="moment",
    )(place, near(before), *late_met)
    came = lax.ppermute(sent, "paths", [(i, i ^ 1) for i in range(lines)])
    own_sum, *sums = pl.pallas_call(
        cores_kernel,
        out_shape=[pltpu.VMEM((CP_DEV, width), jnp.float32)]
        + [pltpu.VMEM((CP_DEV, width), jnp.bfloat16)] * chips,
        in_specs=[SMEM, VMEM, VMEM],
        out_specs=[VMEM] * (chips + 1),
        compiler_params=BIG,
        name="cores",
    )(x[None], near(kept), near(came))

    def flat(p, zz, yy):
        return p * groups + zz * depth + yy

    arrived = []
    for e in range(1, chips):
        arrived.append(lax.ppermute(sums[e], "paths", [(i, (i + e * CORES) % lines) for i in range(lines)]))
    crossed = []
    for e in range(chips):
        pairs = []
        for p in range(lines):
            row = (p + e * CORES) % lines
            for d in range(1, far + 1):
                zz = (row + d) % lines
                pairs += [(flat(p, zz, yy), flat(zz, row, yy)) for yy in range(depth)]
        crossed.append(lax.ppermute(sums[e], ("paths", "cpty"), pairs))
    total, *swaps = pl.pallas_call(
        functools.partial(chips_kernel, count=chips - 1),
        out_shape=[pltpu.VMEM((CP_DEV, CP_DEV), jnp.float32)]
        + [pltpu.VMEM((CP_DEV, CP_DEV), jnp.bfloat16)] * (depth - 1),
        in_specs=[VMEM] * chips,
        out_specs=[VMEM] * depth,
        compiler_params=BIG,
        name="chips",
    )(near(own_sum), *[near(a) for a in arrived])
    swapped = []
    for e in range(1, depth):
        pairs = []
        for p in range(lines):
            for d in range(lines):
                zz = (p + d) % lines
                pairs += [(flat(p, zz, yy), flat(p, zz, (yy - e) % depth)) for yy in range(depth)]
        swapped.append(lax.ppermute(swaps[e - 1], ("paths", "cpty"), pairs))
    moment = pl.pallas_call(
        functools.partial(final_kernel, scale=1.0 / (paths * lines)),
        out_shape=jax.ShapeDtypeStruct((depth, CP_DEV, CP_DEV), jnp.float32),
        in_specs=[SMEM] + [VMEM] * (depth + chips),
        out_specs=VMEM,
        compiler_params=BIG,
        name="final",
    )(y[None], near(total), *[near(a) for a in swapped + crossed])
    return exposure, moment.reshape(depth * CP_DEV, CP_DEV)


def solution(mesh):
    in_specs = (P(None, "paths"), P(None, "cpty"), P("cpty"), P("cpty"), P("cpty"), P("cpty"))
    out_specs = (P("paths", "cpty"), P("paths", "cpty"))
    return jax.shard_map(on_device, mesh=mesh, in_specs=in_specs, out_specs=out_specs, check_vma=False)
```
